32 devices in a mesh: rep: 2 (over y), pipe: 2 (over core), tp: 8 (over z, x).
Axes of the slice: x: 2, y: 2, z: 4, core: 2. Of those that a mesh axis runs over, the one named last changes fastest.
Arguments:
- hidden_entering: bfloat16 [2, 120, 8192], P('rep', None, 'tp'), parts along dimension 0, may hold values from -60 to 60
- segment_adapter: int32 [2, 3], P('rep'), parts along dimension 0, may hold values from 0 to 127, as said below
- segment_requests: int32 [2, 3], P('rep'), parts along dimension 0, may hold values from 10 to 40, as said below
- section_norm_gain: float32 [2, 8192], P('pipe'), may hold values from 0.25 to 1.75
- up_matrix: bfloat16 [2, 14336, 8192], P('pipe', 'tp'), may hold values from -0.0625 to 0.0625
- down_matrix: bfloat16 [2, 8192, 14336], P('pipe', 'tp'), may hold values from -0.046875 to 0.046875
- adapter_reduce: bfloat16 [2, 128, 131072], P('pipe', None, 'tp'), may hold values from -0.0625 to 0.0625
- adapter_expand: bfloat16 [2, 128, 229376], P('pipe', None, 'tp'), may hold values from -1.5 to 1.5
Outputs:
- section_out: bfloat16 [2, 2, 120, 8192], P('pipe', 'rep', None, 'tp'), parts along dimension 1
The draws below stay inside these ranges and needn't reach their ends.
There are 2 independent parts, one for each index of `rep`. The reference program is written for one: setup_inputs(seed, part) draws one part's arguments, and reference() takes and returns one part's arrays. A program takes and returns all parts, laid end to end along the dimension named above; an argument that names none is the same for every part. Nothing has to cross between parts.
Inputs may be any that keep to these rules, and one draw needn't show every extreme that they name: `segment_adapter`: within each micro-batch the adapter ids of its segments do not decrease. The first segment_requests[m, j] rows of segment j of micro-batch m hold requests; the other rows are padding.
All inputs are finite; a program needn't handle non-finite values.
Results may differ from the reference program's by a relative error of at most 0.0045.
Values may be sent and summed in bfloat16 or wider, within the bound.
A program may use at most 128 MiB of HBM per device.

```python
import math
import jax
import jax.numpy as jnp
from jax import lax

MODEL_DIMENSION = 8192
FEEDFORWARD_UNITS = 14336
ADAPTER_RANK = 16
ADAPTER_COUNT = 128
SEG = 40
SPM = 3
MB = 1
N_PIPE = 2


def draw_hidden_entering(key, part):
    row_count = SPM * SEG
    keys = jax.random.split(jax.random.fold_in(key, 101), 3)
    row_scale = jnp.exp(jax.random.uniform(keys[0], (MB, row_count, 1), jnp.float32, math.log(0.4), math.log(4.0)))
    rising = jnp.exp(math.log(3.0) * jnp.arange(MODEL_DIMENSION, dtype=jnp.float32) / MODEL_DIMENSION)
    col_scale = jnp.exp(jax.random.uniform(keys[1], (MODEL_DIMENSION,), jnp.float32, math.log(0.4), math.log(4.0))) * rising / 1.7
    values = jax.random.normal(keys[2], (MB, row_count, MODEL_DIMENSION), jnp.float32)
    return jnp.clip(values * row_scale * col_scale, -60.0, 60.0).astype(jnp.bfloat16)


def draw_segment_adapter(key, part):
    raw = jax.random.randint(jax.random.fold_in(key, 7), (MB, SPM), 0, ADAPTER_COUNT)
    return jnp.sort(raw, axis=-1).astype(jnp.int32)


def draw_segment_requests(key, part):
    keys = jax.random.split(jax.random.fold_in(key, 13), 2)
    counts = jax.random.randint(keys[0], (MB * SPM,), SEG // 4, SEG + 1)
    chosen = jax.random.randint(keys[1], (), 0, MB * SPM)
    counts = jnp.where(jnp.arange(MB * SPM) == chosen, SEG, counts)
    return counts.reshape(MB, SPM).astype(jnp.int32)


def level_of(key, dims, cuts, least, largest):
    def one(position, shards_of):
        steps = jax.random.uniform(jax.random.fold_in(jax.random.fold_in(key, 6), position), (shards_of,), jnp.float32, least / len(cuts), largest / len(cuts))
        return jnp.repeat(jnp.exp(steps), dims[position] // shards_of).reshape((-1,) + (1,) * (len(dims) - position - 1))

    factor_of = one(*cuts[0])
    for cut in cuts[1:]:
        factor_of = factor_of * one(*cut)
    return factor_of


def bell_draw(key, extent, spread, most, shards=(), kind=jnp.bfloat16):
    loudness = level_of(key, extent, shards, -0.22, 0.18) if shards else 1.0
    entries = jax.random.normal(key, extent, jnp.float32) * spread * loudness
    return jnp.minimum(jnp.maximum(entries, -most), most).astype(kind)


def setup_inputs(seed: int = 0, part: int = 0) -> dict:
    seeds = jax.random.split(jax.random.key(seed), 9)
    part_keys = jax.random.split(jax.random.fold_in(seeds[8], part), 9)
    hidden_entering = draw_hidden_entering(jax.random.fold_in(jax.random.fold_in(seeds[8], part), 71), part)
    segment_adapter = draw_segment_adapter(jax.random.fold_in(jax.random.fold_in(seeds[8], part), 71), part)
    segment_requests = draw_segment_requests(jax.random.fold_in(jax.random.fold_in(seeds[8], part), 71), part)
    section_norm_gain = jnp.clip(1.0 + 0.15 * jax.random.normal(seeds[3], (N_PIPE, MODEL_DIMENSION), jnp.float32), 0.25, 1.75)
    up_matrix = bell_draw(seeds[4], (N_PIPE, FEEDFORWARD_UNITS, MODEL_DIMENSION), MODEL_DIMENSION ** -0.5, 0.0625, ((0, 2), (1, 8)))
    down_matrix = bell_draw(seeds[5], (N_PIPE, MODEL_DIMENSION, FEEDFORWARD_UNITS), FEEDFORWARD_UNITS ** -0.5, 0.046875, ((0, 2), (1, 8)))
    adapter_reduce = bell_draw(seeds[6], (N_PIPE, ADAPTER_COUNT, MODEL_DIMENSION * ADAPTER_RANK), MODEL_DIMENSION ** -0.5, 0.0625, ((0, 2), (2, 8)))
    adapter_expand = bell_draw(seeds[7], (N_PIPE, ADAPTER_COUNT, FEEDFORWARD_UNITS * ADAPTER_RANK), ADAPTER_RANK ** -0.5, 1.5, ((0, 2), (2, 8)))
    return dict(hidden_entering=hidden_entering, segment_adapter=segment_adapter, segment_requests=segment_requests, section_norm_gain=section_norm_gain, up_matrix=up_matrix, down_matrix=down_matrix, adapter_reduce=adapter_reduce, adapter_expand=adapter_expand)


EPSILON = 1e-05

def times_rows(left, weight):
    return lax.dot_general(left, weight, (((1,), (1,)), ((), ())), preferred_element_type=jnp.float32)

def apply_section(hidden_flow, section_ordinal, segment_adapter, segment_requests, section_norm_gain, up_matrix, down_matrix, adapter_reduce, adapter_expand):
    batch_list = hidden_flow.shape[0]
    row_count = hidden_flow.shape[1]
    feature_width = hidden_flow.shape[2]
    hidden_extent = up_matrix.shape[1]
    batch_results = segment_adapter.shape[1]
    seg_rows = row_count // batch_results
    adapter_rank_count = adapter_reduce.shape[2] // feature_width
    widened = hidden_flow.astype(jnp.float32)
    scaled = (widened * section_norm_gain[section_ordinal]).astype(jnp.bfloat16)
    inverse = lax.rsqrt(lax.optimization_barrier(jnp.mean(widened * widened, axis=-1, keepdims=True)) + EPSILON)
    flat_scaled = scaled.reshape(batch_list * row_count, feature_width)
    base_up = times_rows(flat_scaled, up_matrix[section_ordinal]).reshape(batch_list, row_count, hidden_extent)
    input_panel = adapter_reduce[section_ordinal][segment_adapter].reshape(batch_list, batch_results, feature_width, adapter_rank_count).astype(jnp.float32)
    output_panel = adapter_expand[section_ordinal][segment_adapter].reshape(batch_list, batch_results, hidden_extent, adapter_rank_count).astype(jnp.float32)
    segment_scaled = scaled.reshape(batch_list, batch_results, seg_rows, feature_width).astype(jnp.float32)
    shrunk = jnp.einsum('msdr,mspd->msrp', input_panel, segment_scaled)
    low_rank = (inverse.reshape(batch_list, batch_results, 1, seg_rows) * shrunk).astype(jnp.bfloat16)
    adapted = jnp.einsum('msrp,msdr->mspd', low_rank.astype(jnp.float32), output_panel).reshape(batch_list, row_count, hidden_extent)
    up_sum = inverse * base_up + adapted
    hidden_act = jax.nn.silu(up_sum).astype(jnp.bfloat16)
    down_sum = times_rows(hidden_act.reshape(batch_list * row_count, hidden_extent), down_matrix[section_ordinal]).reshape(batch_list, row_count, feature_width)
    updated = (widened + down_sum).astype(jnp.bfloat16)
    positions = lax.broadcasted_iota(jnp.int32, (batch_list, batch_results, seg_rows), 2)
    row_kept = (positions < segment_requests[:, :, None]).reshape(batch_list, row_count, 1)
    return jnp.where(row_kept, updated, jnp.zeros_like(updated))

def reference(hidden_entering, segment_adapter, segment_requests, section_norm_gain, up_matrix, down_matrix, adapter_reduce, adapter_expand):
    hidden_flow = hidden_entering
    outputs = []
    for section_ordinal in range(N_PIPE):
        hidden_flow = apply_section(hidden_flow, section_ordinal, segment_adapter, segment_requests, section_norm_gain, up_matrix, down_matrix, adapter_reduce, adapter_expand)
        outputs.append(hidden_flow)
    return jnp.stack(outputs)
```

```python
import functools

import jax
import jax.numpy as jnp
from jax import lax
from jax.experimental import pallas as pl
from jax.experimental.pallas import tpu as pltpu
from jax.sharding import PartitionSpec as P

EPSILON = 1e-05


def shifted(x, axis, by):
    size = lax.axis_size(axis)
    pairs = [(i, i + by) for i in range(size) if 0 <= i + by < size]
    return lax.ppermute(x, axis, pairs)


def times_rows(left, weight):
    return lax.dot_general(
        left, weight, (((1,), (1,)), ((), ())), preferred_element_type=jnp.float32
    )


def block_step(
    current, unit_ids, unit_live, gain_full, up_weight, down_weight, shrink_weight, expand_weight
):
    row_count = current.shape[0]
    col_count = current.shape[1]
    hid_count = up_weight.shape[0]
    segments = unit_ids.shape[0]
    seg_rows = row_count // segments
    feature_width = gain_full.shape[0]
    adapter_rank_count = shrink_weight.shape[1] // col_count
    column = lax.axis_index("tp") * col_count
    gain_mine = lax.dynamic_slice_in_dim(gain_full, column, col_count, 0)
    widened_local = current.astype(jnp.float32)
    local_scaled = (widened_local * gain_mine).astype(jnp.bfloat16)
    input_panel = shrink_weight[unit_ids].reshape(segments, col_count, adapter_rank_count)
    output_panel = expand_weight[unit_ids].reshape(segments, hid_count, adapter_rank_count)
    partial_value = jnp.einsum(
        "sdr,spd->rsp",
        input_panel,
        local_scaled.reshape(segments, seg_rows, col_count),
        preferred_element_type=jnp.float32,
    ).reshape(adapter_rank_count, row_count)
    local_squares = jnp.sum(widened_local * widened_local, axis=1)
    reduced, squares = lax.psum((partial_value, local_squares), "tp")
    widened = lax.all_gather(current, "tp", axis=1, tiled=True).astype(jnp.float32)
    scaled = (widened * gain_full).astype(jnp.bfloat16)
    up_total = times_rows(scaled, up_weight)
    inverse = lax.rsqrt(squares / feature_width + EPSILON)
    low_rank = (
        (reduced * inverse[None, :])
        .astype(jnp.bfloat16)
        .reshape(adapter_rank_count, segments, seg_rows)
    )
    adapted = jnp.einsum(
        "rsp,sdr->spd", low_rank, output_panel, preferred_element_type=jnp.float32
    ).reshape(row_count, hid_count)
    up_sum = inverse[:, None] * up_total + adapted
    hidden_act = jax.nn.silu(up_sum).astype(jnp.bfloat16)
    down_sum = times_rows(lax.all_gather(hidden_act, "tp", axis=1, tiled=True), down_weight)
    updated = (widened_local + down_sum).astype(jnp.bfloat16)
    positions = lax.broadcasted_iota(jnp.int32, (segments, seg_rows), 1)
    row_kept = (positions < unit_live[:, None]).reshape(row_count, 1)
    return jnp.where(row_kept, updated, jnp.zeros_like(updated))


MESH = pl.DeviceIdType.MESH
PIECE = 256
COLUMNS = 2
VMEM_BYTES = 67_043_328


def section_kernel(
    x_ref, gain_ref, keep_ref, reduce_ref, expand_ref, up_hbm, down_hbm, out_ref,
    up_v, down_v, xs, act, current, acc, partial,
    up_sem, down_sem, part_send, part_recv, x_send, x_recv, a_send, a_recv, pipe_sem,
):
    shards, x_pieces, rows, _ = xs.shape
    a_pieces = act.shape[1]
    cols = x_ref.shape[1]
    hidden = up_v.shape[0]
    width = shards * cols
    segments = reduce_ref.shape[0]
    rank = reduce_ref.shape[1]
    seg_rows = rows // segments
    depth = shards // COLUMNS
    me = lax.axis_index("tp")
    stage = lax.axis_index("pipe")
    stages = lax.axis_size("pipe")
    z, x = me // COLUMNS, me % COLUMNS
    partner = z * COLUMNS + (1 - x)

    def up_copy(c):
        span = pl.ds(c * PIECE, PIECE)
        return pltpu.make_async_copy(up_hbm.at[span, :], up_v.at[span, :], up_sem.at[c])

    def down_copy(t):
        span = pl.ds(pl.multiple_of(t * hidden, 128), hidden)
        return pltpu.make_async_copy(down_hbm.at[:, span], down_v.at[:, span], down_sem.at[t])

    @pl.loop(0, a_pieces)
    def _(c):
        up_copy(c).start()

    @pl.loop(0, shards)
    def _(i):
        down_copy((me + i) % shards).start()

    barrier = pltpu.get_barrier_semaphore()

    @pl.loop(1, shards)
    def _(i):
        pl.semaphore_signal(barrier, inc=1, device_id={"tp": (me + i) % shards}, device_id_type=MESH)

    @pl.when(stage > 0)
    def _():
        pl.semaphore_signal(barrier, inc=1, device_id={"pipe": stage - 1}, device_id_type=MESH)

    @pl.when(stage < stages - 1)
    def _():
        pl.semaphore_signal(barrier, inc=1, device_id={"pipe": stage + 1}, device_id_type=MESH)

    neighbours = jnp.where(stage > 0, 1, 0) + jnp.where(stage < stages - 1, 1, 0)
    pl.semaphore_wait(barrier, shards - 1 + neighbours)

    def hand_over():
        return pltpu.make_async_remote_copy(
            src_ref=out_ref, dst_ref=current, send_sem=pipe_sem.at[0], recv_sem=pipe_sem.at[1],
            device_id={"pipe": (stage + 1) % stages}, device_id_type=MESH)

    @pl.when(stage == 0)
    def _():
        current[...] = x_ref[...]

    @pl.when(stage > 0)
    def _():
        hand_over().wait_recv()

    class Spread:
        def __init__(self, buf, send, recv, pieces):
            self.buf, self.send, self.recv, self.pieces = buf, send, recv, pieces

        def copy(self, t, c, way, target):
            return pltpu.make_async_remote_copy(
                src_ref=self.buf.at[t, c], dst_ref=self.buf.at[t, c],
                send_sem=self.send.at[way, t, c], recv_sem=self.recv.at[t, c],
                device_id={"tp": target}, device_id_type=MESH)

        def each(self, source_z, c, do):
            t = source_z * COLUMNS + x

            @pl.when(jnp.logical_and(source_z <= z, z < depth - 1))
            def _():
                do(self.copy(t, c, 0, (me + COLUMNS) % shards))

            @pl.when(jnp.logical_and(source_z >= z, z > 0))
            def _():
                do(self.copy(t, c, 1, (me + shards - COLUMNS) % shards))

            do(self.copy(t, c, 2, partner))

        def forward(self, source_z, c):
            self.each(source_z, c, lambda d: d.start())

        def arrive(self, t, c):
            self.copy(t, c, 2, partner).wait_recv()

        def relay(self, step, c):
            @pl.when(z >= step)
            def _():
                self.arrive((z - step) * COLUMNS + x, c)
                self.forward(z - step, c)

            @pl.when(z + step < depth)
            def _():
                self.arrive((z + step) * COLUMNS + x, c)
                self.forward(z + step, c)

        def partner_arrive(self, t):
            @pl.loop(0, self.pieces)
            def _(c):
                self.arrive(t, c)

        def drain(self):
            @pl.loop(0, depth)
            def _(source_z):
                @pl.loop(0, self.pieces)
                def _(c):
                    self.each(source_z, c, lambda d: d.wait_send())

    x_side = Spread(xs, x_send, x_recv, x_pieces)
    a_side = Spread(act, a_send, a_recv, a_pieces)

    for c in range(x_pieces):
        gain = gain_ref[:, pl.ds(pl.multiple_of(me * cols + c * PIECE, 128), PIECE)]
        wide = current[:, c * PIECE:(c + 1) * PIECE].astype(jnp.float32)
        xs[me, c] = (wide * gain).astype(jnp.bfloat16)
        x_side.forward(z, c)

    lane_seg = lax.broadcasted_iota(jnp.int32, (1, 128), 1) // seg_rows
    nt = (((1,), (1,)), ((), ()))
    total = jnp.zeros((segments * rank, 128), jnp.float32)
    squares = jnp.zeros((8, 128), jnp.float32)
    lane_pad = 128 - rows
    for c in range(x_pieces):
        span = slice(c * PIECE, (c + 1) * PIECE)
        mine = jnp.concatenate([xs[me, c], jnp.zeros((lane_pad, PIECE), jnp.bfloat16)], axis=0) if lane_pad else xs[me, c]
        panel = reduce_ref[:, :, span].reshape(segments * rank, PIECE)
        total += lax.dot_general(panel, mine, nt, preferred_element_type=jnp.float32)
        wide = current[:, span].astype(jnp.float32)
        square = wide * wide
        if lane_pad:
            square = jnp.concatenate([square, jnp.zeros((lane_pad, PIECE), jnp.float32)], axis=0)
        squares += lax.dot_general(jnp.ones((8, PIECE), jnp.float32), square, nt,
                                   precision=lax.Precision.HIGHEST, preferred_element_type=jnp.float32)
    picked = jnp.zeros((rank, 128), jnp.float32)
    for s in range(segments):
        picked += jnp.where(lane_seg == s, total[s * rank:(s + 1) * rank], 0.0)
    partial[me, 0:rank] = picked
    partial[me, rank:rank + 8] = squares

    def part_copy(owner, target):
        return pltpu.make_async_remote_copy(
            src_ref=partial.at[owner], dst_ref=partial.at[owner], send_sem=part_send.at[target],
            recv_sem=part_recv.at[owner], device_id={"tp": target}, device_id_type=MESH)

    @pl.loop(1, shards)
    def _(i):
        part_copy(me, (me + i) % shards).start()

    for step in range(1, depth):
        @pl.loop(0, x_pieces)
        def _(c):
            x_side.relay(step, c)

    @pl.loop(1, shards)
    def _(i):
        owner = (me + i) % shards
        part_copy(owner, owner).wait_recv()

    summed = partial[0]
    for t in range(1, shards):
        summed = summed + partial[t]
    inverse_lane = lax.rsqrt(summed[rank:rank + 1] / width + EPSILON)
    low_lane = (summed[0:rank] * inverse_lane).astype(jnp.bfloat16).astype(jnp.float32)
    blocks = [jnp.where(lane_seg == s, low_lane, 0.0) for s in range(segments)]
    blocks.append(jnp.broadcast_to(inverse_lane, (8, 128)))
    blocks.append(jnp.zeros((128 - segments * rank - 8, 128), jnp.float32))
    turned = jnp.transpose(jnp.concatenate(blocks, axis=0))[:rows]
    low_rank = turned[:, :segments * rank].astype(jnp.bfloat16)
    inverse = turned[:, segments * rank:segments * rank + 1]

    @pl.loop(0, depth)
    def _(source_z):
        x_side.partner_arrive(source_z * COLUMNS + (1 - x))

    LAG = 2

    def relays(k):
        for step in range(1, depth):
            c = k - LAG * step

            @pl.when(jnp.logical_and(c >= 0, c < a_pieces))
            def _():
                a_side.relay(step, c)

    @pl.loop(0, a_pieces)
    def _(k):
        up_copy(k).wait()
        span = pl.ds(pl.multiple_of(k * PIECE, PIECE), PIECE)
        base = jnp.zeros((rows, PIECE), jnp.float32)
        for t in range(shards):
            for c in range(x_pieces):
                at = t * cols + c * PIECE
                base += lax.dot_general(xs[t, c], up_v[span, at:at + PIECE], nt, preferred_element_type=jnp.float32)
        panel = expand_ref[:, :, span].reshape(segments * rank, PIECE)
        adapted = jnp.dot(low_rank, panel, preferred_element_type=jnp.float32)
        value = inverse * base + adapted
        act[me, k] = (value / (1.0 + jnp.exp(-value))).astype(jnp.bfloat16)
        a_side.forward(z, k)
        relays(k)

    acc[...] = current[...].astype(jnp.float32)

    def down_part(t):
        down_copy(t).wait()

        @pl.loop(0, cols // PIECE)
        def _(n):
            block = pl.ds(pl.multiple_of(n * PIECE, PIECE), PIECE)
            part = acc[:, block]
            for c in range(a_pieces):
                span = pl.ds(pl.multiple_of(t * hidden + c * PIECE, 128), PIECE)
                part += lax.dot_general(act[t, c], down_v[block, span], nt, preferred_element_type=jnp.float32)
            acc[:, block] = part

    def down_at(z_of, column):
        @pl.when(jnp.logical_and(z_of >= 0, z_of < depth))
        def _():
            t = z_of * COLUMNS + column

            @pl.when(column != x)
            def _():
                a_side.partner_arrive(t)

            down_part(t)

    order = [(0, 0), (0, 1), (1, 0), (-1, 0), (2, 0), (-2, 0)]
    rest = [(d * sign, o) for d in range(1, depth) for o in (0, 1) for sign in (1, -1)]
    rest = [item for item in rest if item not in order]
    ticks = LAG * (depth - 1)
    for j in range(ticks):
        relays(a_pieces + j)
        if j < len(order):
            far, other = order[j]
            down_at(z + far, (x + other) % COLUMNS)
    for far, other in order[ticks:] + rest:
        down_at(z + far, (x + other) % COLUMNS)

    out_ref[...] = jnp.where(keep_ref[...] > 0.0, acc[...], 0.0).astype(jnp.bfloat16)

    @pl.when(stage < stages - 1)
    def _():
        copy = hand_over()
        copy.start()
        copy.wait_send()

    @pl.loop(1, shards)
    def _(i):
        part_copy(me, (me + i) % shards).wait_send()

    x_side.drain()
    a_side.drain()


def fused_sections(current, ids, live, gain, up_weight, down_weight, shrink_weight, expand_weight):
    rows, cols = current.shape
    hidden = up_weight.shape[0]
    segments = ids.shape[0]
    shards = lax.axis_size("tp")
    rank = shrink_weight.shape[1] // cols

    def panels(table, length):
        picked = [lax.dynamic_slice_in_dim(table, ids[s], 1, 0) for s in range(segments)]
        return jnp.concatenate(picked, axis=0).reshape(segments, length, rank).transpose(0, 2, 1)

    positions = lax.broadcasted_iota(jnp.int32, (segments, rows // segments), 1)
    keep = (positions < live[:, None]).reshape(rows, 1).astype(jnp.float32)
    x_pieces, a_pieces = cols // PIECE, hidden // PIECE
    vmem = pl.BlockSpec(memory_space=pltpu.VMEM)
    hbm = pl.BlockSpec(memory_space=pl.ANY)
    dma = pltpu.SemaphoreType.DMA
    return pl.pallas_call(
        section_kernel,
        out_shape=jax.ShapeDtypeStruct((rows, cols), jnp.bfloat16),
        in_specs=[vmem] * 5 + [hbm] * 2,
        out_specs=vmem,
        scratch_shapes=[
            pltpu.VMEM(up_weight.shape, jnp.bfloat16),
            pltpu.VMEM(down_weight.shape, jnp.bfloat16),
            pltpu.VMEM((shards, x_pieces, rows, PIECE), jnp.bfloat16),
            pltpu.VMEM((shards, a_pieces, rows, PIECE), jnp.bfloat16),
            pltpu.VMEM((rows, cols), jnp.bfloat16),
            pltpu.VMEM((rows, cols), jnp.float32),
            pltpu.VMEM((shards, rank + 8, 128), jnp.float32),
            dma((a_pieces,)), dma((shards,)),
            dma((shards,)), dma((shards,)),
            dma((3, shards, x_pieces)), dma((shards, x_pieces)),
            dma((3, shards, a_pieces)), dma((shards, a_pieces)),
            dma((2,)),
        ],
        compiler_params=pltpu.CompilerParams(
            collective_id=0, has_side_effects=True, vmem_limit_bytes=VMEM_BYTES
        ),
    )(current, gain[None, :], keep, panels(shrink_weight, cols), panels(expand_weight, hidden),
      up_weight, down_weight)


def run_window(
    units, unit_ids, unit_live, gain_full, up_weight, down_weight, shrink_weight, expand_weight
):
    section_index = lax.axis_index("pipe")
    sections = lax.axis_size("pipe")
    unit_count = units.shape[0]
    tick_total = unit_count + sections - 1

    def process(tick_index, received, collected):
        position = jnp.clip(tick_index - section_index, 0, unit_count - 1)
        arriving = lax.dynamic_index_in_dim(
            units, jnp.minimum(tick_index, unit_count - 1), 0, keepdims=False
        )
        current = jnp.where(section_index == 0, arriving, received)
        ids_here = lax.dynamic_index_in_dim(unit_ids, position, 0, keepdims=False)
        live_here = lax.dynamic_index_in_dim(unit_live, position, 0, keepdims=False)
        produced = block_step(
            current,
            ids_here,
            live_here,
            gain_full,
            up_weight,
            down_weight,
            shrink_weight,
            expand_weight,
        )
        lag = tick_index - section_index
        in_window = jnp.logical_and(lag >= 0, lag < unit_count)
        placed = lax.dynamic_update_index_in_dim(collected, produced, position, 0)
        return (produced, jnp.where(in_window, placed, collected))

    def one_tick(tick_index, state):
        produced, collected = process(tick_index, state[0], state[1])
        return (shifted(produced, "pipe", 1), collected)

    start_state = (jnp.zeros_like(units[0]), jnp.zeros_like(units))
    received, collected = lax.fori_loop(0, tick_total - 1, one_tick, start_state)
    produced, collected = process(tick_total - 1, received, collected)
    return collected


def per_device(
    hidden_entering,
    segment_adapter,
    segment_requests,
    section_norm_gain,
    up_matrix,
    down_matrix,
    adapter_reduce,
    adapter_expand,
):
    batch_list = hidden_entering.shape[0]
    row_count = hidden_entering.shape[1]
    col_count = hidden_entering.shape[2]
    hidden = up_matrix.shape[1]
    fits = 2 * hidden * col_count * 2 * lax.axis_size("tp") < VMEM_BYTES - 7 * 2**20
    whole_pieces = col_count % PIECE == 0 and hidden % PIECE == 0
    if batch_list == 1 and whole_pieces and fits and row_count <= 128:
        produced = fused_sections(
            hidden_entering[0],
            segment_adapter[0],
            segment_requests[0],
            section_norm_gain[0],
            up_matrix[0],
            down_matrix[0],
            adapter_reduce[0],
            adapter_expand[0],
        )
        return produced.reshape(1, batch_list, row_count, col_count)
    collected = run_window(
        hidden_entering,
        segment_adapter,
        segment_requests,
        section_norm_gain[0],
        up_matrix[0],
        down_matrix[0],
        adapter_reduce[0],
        adapter_expand[0],
    )
    return collected.reshape(1, batch_list, row_count, col_count)


def solution(mesh):
    return jax.shard_map(
        per_device,
        mesh=mesh,
        in_specs=(
            P("rep", None, "tp"),
            P("rep", None),
            P("rep", None),
            P("pipe", None),
            P("pipe", "tp", None),
            P("pipe", "tp", None),
            P("pipe", None, "tp"),
            P("pipe", None, "tp"),
        ),
        out_specs=P("pipe", "rep", None, "tp"),
        check_vma=False,
    )
```

```python
import functools

import jax
import jax.numpy as jnp
from jax import lax
from jax.experimental import pallas as pl
from jax.experimental.pallas import tpu as pltpu
from jax.sharding import PartitionSpec as P

EPSILON = 1e-05


def shifted(x, axis, by):
    size = lax.axis_size(axis)
    pairs = [(i, i + by) for i in range(size) if 0 <= i + by < size]
    return lax.ppermute(x, axis, pairs)


def times_rows(left, weight):
    return lax.dot_general(
        left, weight, (((1,), (1,)), ((), ())), preferred_element_type=jnp.float32
    )


def block_step(
    current, unit_ids, unit_live, gain_full, up_weight, down_weight, shrink_weight, expand_weight
):
    row_count = current.shape[0]
    col_count = current.shape[1]
    hid_count = up_weight.shape[0]
    segments = unit_ids.shape[0]
    seg_rows = row_count // segments
    feature_width = gain_full.shape[0]
    adapter_rank_count = shrink_weight.shape[1] // col_count
    column = lax.axis_index("tp") * col_count
    gain_mine = lax.dynamic_slice_in_dim(gain_full, column, col_count, 0)
    widened_local = current.astype(jnp.float32)
    local_scaled = (widened_local * gain_mine).astype(jnp.bfloat16)
    input_panel = shrink_weight[unit_ids].reshape(segments, col_count, adapter_rank_count)
    output_panel = expand_weight[unit_ids].reshape(segments, hid_count, adapter_rank_count)
    partial_value = jnp.einsum(
        "sdr,spd->rsp",
        input_panel,
        local_scaled.reshape(segments, seg_rows, col_count),
        preferred_element_type=jnp.float32,
    ).reshape(adapter_rank_count, row_count)
    local_squares = jnp.sum(widened_local * widened_local, axis=1)
    reduced, squares = lax.psum((partial_value, local_squares), "tp")
    widened = lax.all_gather(current, "tp", axis=1, tiled=True).astype(jnp.float32)
    scaled = (widened * gain_full).astype(jnp.bfloat16)
    up_total = times_rows(scaled, up_weight)
    inverse = lax.rsqrt(squares / feature_width + EPSILON)
    low_rank = (
        (reduced * inverse[None, :])
        .astype(jnp.bfloat16)
        .reshape(adapter_rank_count, segments, seg_rows)
    )
    adapted = jnp.einsum(
        "rsp,sdr->spd", low_rank, output_panel, preferred_element_type=jnp.float32
    ).reshape(row_count, hid_count)
    up_sum = inverse[:, None] * up_total + adapted
    hidden_act = jax.nn.silu(up_sum).astype(jnp.bfloat16)
    down_sum = times_rows(lax.all_gather(hidden_act, "tp", axis=1, tiled=True), down_weight)
    updated = (widened_local + down_sum).astype(jnp.bfloat16)
    positions = lax.broadcasted_iota(jnp.int32, (segments, seg_rows), 1)
    row_kept = (positions < unit_live[:, None]).reshape(row_count, 1)
    return jnp.where(row_kept, updated, jnp.zeros_like(updated))


MESH = pl.DeviceIdType.MESH
PIECE = 256
COLUMNS = 2
VMEM_BYTES = 67_043_328


def section_kernel(
    live_ref, x_ref, gain_ref, reduce_ref, expand_ref, up_hbm, down_hbm, out_ref,
    up_v, down_v, xs, act, current, acc, partial,
    up_sem, down_sem, part_send, part_recv, x_send, x_recv, a_send, a_recv, pipe_sem,
):
    shards, x_pieces, rows, _ = xs.shape
    a_pieces = act.shape[1]
    cols = x_ref.shape[1]
    hidden = up_v.shape[0]
    width = shards * cols
    segments = reduce_ref.shape[0]
    rank = reduce_ref.shape[1]
    seg_rows = rows // segments
    depth = shards // COLUMNS
    me = lax.axis_index("tp")
    stage = lax.axis_index("pipe")
    stages = lax.axis_size("pipe")
    z, x = me // COLUMNS, me % COLUMNS
    partner = z * COLUMNS + (1 - x)

    def up_copy(c):
        span = pl.ds(c * PIECE, PIECE)
        return pltpu.make_async_copy(up_hbm.at[span, :], up_v.at[span, :], up_sem.at[c])

    def down_copy(t):
        span = pl.ds(pl.multiple_of(t * hidden, 128), hidden)
        return pltpu.make_async_copy(down_hbm.at[:, span], down_v.at[:, span], down_sem.at[t])

    @pl.loop(0, a_pieces)
    def _(c):
        up_copy(c).start()

    @pl.loop(0, shards)
    def _(i):
        down_copy((me + i) % shards).start()

    barrier = pltpu.get_barrier_semaphore()

    @pl.loop(1, shards)
    def _(i):
        pl.semaphore_signal(barrier, inc=1, device_id={"tp": (me + i) % shards}, device_id_type=MESH)

    @pl.when(stage > 0)
    def _():
        pl.semaphore_signal(barrier, inc=1, device_id={"pipe": stage - 1}, device_id_type=MESH)

    @pl.when(stage < stages - 1)
    def _():
        pl.semaphore_signal(barrier, inc=1, device_id={"pipe": stage + 1}, device_id_type=MESH)

    neighbours = jnp.where(stage > 0, 1, 0) + jnp.where(stage < stages - 1, 1, 0)
    pl.semaphore_wait(barrier, shards - 1 + neighbours)

    def hand_over():
        return pltpu.make_async_remote_copy(
            src_ref=out_ref, dst_ref=current, send_sem=pipe_sem.at[0], recv_sem=pipe_sem.at[1],
            device_id={"pipe": (stage + 1) % stages}, device_id_type=MESH)

    @pl.when(stage == 0)
    def _():
        current[...] = x_ref[...]

    @pl.when(stage > 0)
    def _():
        hand_over().wait_recv()

    class Spread:
        def __init__(self, buf, send, recv, pieces):
            self.buf, self.send, self.recv, self.pieces = buf, send, recv, pieces

        def copy(self, t, c, way, target):
            return pltpu.make_async_remote_copy(
                src_ref=self.buf.at[t, c], dst_ref=self.buf.at[t, c],
                send_sem=self.send.at[way, t, c], recv_sem=self.recv.at[t, c],
                device_id={"tp": target}, device_id_type=MESH)

        def each(self, source_z, column, c, do):
            t = source_z * COLUMNS + column
            own, first = column == x, c == 0
            along = jnp.logical_or(own, first)
            across = jnp.logical_and(own, jnp.logical_or(c != 0, source_z == z))

            @pl.when(jnp.logical_and(along, jnp.logical_and(source_z <= z, z < depth - 1)))
            def _():
                do(self.copy(t, c, 0, (me + COLUMNS) % shards))

            @pl.when(jnp.logical_and(along, jnp.logical_and(source_z >= z, z > 0)))
            def _():
                do(self.copy(t, c, 1, (me + shards - COLUMNS) % shards))

            @pl.when(across)
            def _():
                do(self.copy(t, c, 2, partner))

        def forward(self, source_z, column, c):
            self.each(source_z, column, c, lambda d: d.start())

        def arrive(self, t, c):
            self.copy(t, c, 2, partner).wait_recv()

        def pass_on(self, source_z, column, c):
            @pl.when(jnp.logical_and(source_z >= 0, source_z < depth))
            def _():
                self.arrive(source_z * COLUMNS + column, c)
                self.forward(source_z, column, c)

        def relay(self, step, column, c):
            for source_z in (z - step, z + step) if step else (z,):
                self.pass_on(source_z, column, c)

        def partner_arrive(self, t):
            @pl.loop(1, self.pieces)
            def _(c):
                self.arrive(t, c)

        def drain(self):
            @pl.loop(0, depth)
            def _(source_z):
                @pl.loop(0, self.pieces)
                def _(c):
                    self.each(source_z, x, c, lambda d: d.wait_send())

                self.each(source_z, 1 - x, 0, lambda d: d.wait_send())

    x_side = Spread(xs, x_send, x_recv, x_pieces)
    a_side = Spread(act, a_send, a_recv, a_pieces)

    for c in range(x_pieces):
        gain = gain_ref[:, pl.ds(pl.multiple_of(me * cols + c * PIECE, 128), PIECE)]
        wide = current[:, c * PIECE:(c + 1) * PIECE].astype(jnp.float32)
        xs[me, c] = (wide * gain).astype(jnp.bfloat16)
        x_side.forward(z, x, c)

    lane_seg = lax.broadcasted_iota(jnp.int32, (1, 128), 1) // seg_rows
    nt = (((1,), (1,)), ((), ()))
    total = jnp.zeros((segments * rank, 128), jnp.float32)
    squares = jnp.zeros((8, 128), jnp.float32)
    lane_pad = 128 - rows
    for c in range(x_pieces):
        span = slice(c * PIECE, (c + 1) * PIECE)
        mine = jnp.concatenate([xs[me, c], jnp.zeros((lane_pad, PIECE), jnp.bfloat16)], axis=0) if lane_pad else xs[me, c]
        panel = reduce_ref[:, :, span].reshape(segments * rank, PIECE)
        total += lax.dot_general(panel, mine, nt, preferred_element_type=jnp.float32)
        wide = current[:, span].astype(jnp.float32)
        square = wide * wide
        if lane_pad:
            square = jnp.concatenate([square, jnp.zeros((lane_pad, PIECE), jnp.float32)], axis=0)
        squares += lax.dot_general(jnp.ones((8, PIECE), jnp.float32), square, nt,
                                   precision=lax.Precision.HIGHEST, preferred_element_type=jnp.float32)
    picked = jnp.zeros((rank, 128), jnp.float32)
    for s in range(segments):
        picked += jnp.where(lane_seg == s, total[s * rank:(s + 1) * rank], 0.0)
    partial[me, 0:rank] = picked
    partial[me, rank:rank + 8] = squares

    def part_copy(owner, target):
        return pltpu.make_async_remote_copy(
            src_ref=partial.at[owner], dst_ref=partial.at[owner], send_sem=part_send.at[target],
            recv_sem=part_recv.at[owner], device_id={"tp": target}, device_id_type=MESH)

    @pl.loop(1, shards)
    def _(i):
        part_copy(me, (me + i) % shards).start()

    x_side.relay(0, 1 - x, 0)
    for step in range(1, depth):
        @pl.loop(0, x_pieces)
        def _(c):
            x_side.relay(step, x, c)

        x_side.relay(step, 1 - x, 0)

    @pl.loop(1, shards)
    def _(i):
        owner = (me + i) % shards
        part_copy(owner, owner).wait_recv()

    summed = partial[0]
    for t in range(1, shards):
        summed = summed + partial[t]
    inverse_lane = lax.rsqrt(summed[rank:rank + 1] / width + EPSILON)
    low_lane = (summed[0:rank] * inverse_lane).astype(jnp.bfloat16).astype(jnp.float32)
    blocks = [jnp.where(lane_seg == s, low_lane, 0.0) for s in range(segments)]
    blocks.append(jnp.broadcast_to(inverse_lane, (8, 128)))
    blocks.append(jnp.zeros((128 - segments * rank - 8, 128), jnp.float32))
    turned = jnp.transpose(jnp.concatenate(blocks, axis=0))[:rows]
    low_rank = turned[:, :segments * rank].astype(jnp.bfloat16)
    inverse = turned[:, segments * rank:segments * rank + 1]

    @pl.loop(0, depth)
    def _(source_z):
        x_side.partner_arrive(source_z * COLUMNS + (1 - x))

    LAG = 3

    def relays(k):
        for step in range(1, depth):
            c = k - LAG * step

            @pl.when(jnp.logical_and(c >= 0, c < a_pieces))
            def _():
                a_side.relay(step, x, c)

        for step in range(depth):
            @pl.when(k == LAG * (step + 1))
            def _():
                a_side.relay(step, 1 - x, 0)

    @pl.loop(0, a_pieces)
    def _(k):
        up_copy(k).wait()
        span = pl.ds(pl.multiple_of(k * PIECE, PIECE), PIECE)
        base = jnp.zeros((rows, PIECE), jnp.float32)
        for t in range(shards):
            for c in range(x_pieces):
                at = t * cols + c * PIECE
                base += lax.dot_general(xs[t, c], up_v[span, at:at + PIECE], nt, preferred_element_type=jnp.float32)
        panel = expand_ref[:, :, span].reshape(segments * rank, PIECE)
        adapted = jnp.dot(low_rank, panel, preferred_element_type=jnp.float32)
        value = inverse * base + adapted
        act[me, k] = (value / (1.0 + jnp.exp(-value))).astype(jnp.bfloat16)
        a_side.forward(z, x, k)
        relays(k)

    acc[...] = current[...].astype(jnp.float32)

    def down_part(t):
        down_copy(t).wait()

        @pl.loop(0, cols // PIECE)
        def _(n):
            block = pl.ds(pl.multiple_of(n * PIECE, PIECE), PIECE)
            part = acc[:, block]
            for c in range(a_pieces):
                span = pl.ds(pl.multiple_of(t * hidden + c * PIECE, 128), PIECE)
                part += lax.dot_general(act[t, c], down_v[block, span], nt, preferred_element_type=jnp.float32)
            acc[:, block] = part

    def down_at(z_of, column):
        @pl.when(jnp.logical_and(z_of >= 0, z_of < depth))
        def _():
            t = z_of * COLUMNS + column

            @pl.when(column != x)
            def _():
                a_side.partner_arrive(t)

            down_part(t)

    order = [[(0, 0)], [(0, 1)], [(1, 0)], [(-1, 0)], [(1, 1), (-1, 1)], [(2, 0), (-2, 0)], [(2, 1), (-2, 1)], [], []]
    begun = [item for items in order for item in items]
    rest = [(d * sign, o) for d in range(1, depth) for o in (0, 1) for sign in (1, -1)]
    ticks = LAG * (depth - 1)
    order += [[item for item in rest if item not in begun]]
    for j in range(max(ticks, len(order))):
        if j < ticks:
            relays(a_pieces + j)
        for far, other in order[j] if j < len(order) else ():
            down_at(z + far, (x + other) % COLUMNS)

    row = lax.broadcasted_iota(jnp.int32, (rows, 1), 0)
    kept = row < 0
    for s in range(segments):
        low = s * seg_rows
        kept = jnp.logical_or(kept, jnp.logical_and(row >= low, row < low + jnp.minimum(live_ref[s], seg_rows)))
    out_ref[...] = jnp.where(kept, acc[...], 0.0).astype(jnp.bfloat16)

    @pl.when(stage < stages - 1)
    def _():
        copy = hand_over()
        copy.start()
        copy.wait_send()

    @pl.loop(1, shards)
    def _(i):
        part_copy(me, (me + i) % shards).wait_send()

    x_side.drain()
    a_side.drain()


def fused_sections(current, ids, live, gain, up_weight, down_weight, shrink_weight, expand_weight):
    rows, cols = current.shape
    hidden = up_weight.shape[0]
    segments = ids.shape[0]
    shards = lax.axis_size("tp")
    rank = shrink_weight.shape[1] // cols

    def panels(table, length):
        picked = [lax.dynamic_slice_in_dim(table, ids[s], 1, 0) for s in range(segments)]
        return jnp.concatenate(picked, axis=0).reshape(segments, length, rank).transpose(0, 2, 1)

    x_pieces, a_pieces = cols // PIECE, hidden // PIECE
    vmem = pl.BlockSpec(memory_space=pltpu.VMEM)
    hbm = pl.BlockSpec(memory_space=pl.ANY)
    dma = pltpu.SemaphoreType.DMA
    return pl.pallas_call(
        section_kernel,
        out_shape=jax.ShapeDtypeStruct((rows, cols), jnp.bfloat16),
        in_specs=[pl.BlockSpec(memory_space=pltpu.SMEM)] + [vmem] * 4 + [hbm] * 2,
        out_specs=vmem,
        scratch_shapes=[
            pltpu.VMEM(up_weight.shape, jnp.bfloat16),
            pltpu.VMEM(down_weight.shape, jnp.bfloat16),
            pltpu.VMEM((shards, x_pieces, rows, PIECE), jnp.bfloat16),
            pltpu.VMEM((shards, a_pieces, rows, PIECE), jnp.bfloat16),
            pltpu.VMEM((rows, cols), jnp.bfloat16),
            pltpu.VMEM((rows, cols), jnp.float32),
            pltpu.VMEM((shards, rank + 8, 128), jnp.float32),
            dma((a_pieces,)), dma((shards,)),
            dma((shards,)), dma((shards,)),
            dma((3, shards, x_pieces)), dma((shards, x_pieces)),
            dma((3, shards, a_pieces)), dma((shards, a_pieces)),
            dma((2,)),
        ],
        compiler_params=pltpu.CompilerParams(
            collective_id=0, has_side_effects=True, vmem_limit_bytes=VMEM_BYTES
        ),
    )(live, current, gain[None, :], panels(shrink_weight, cols), panels(expand_weight, hidden),
      up_weight, down_weight)


def run_window(
    units, unit_ids, unit_live, gain_full, up_weight, down_weight, shrink_weight, expand_weight
):
    section_index = lax.axis_index("pipe")
    sections = lax.axis_size("pipe")
    unit_count = units.shape[0]
    tick_total = unit_count + sections - 1

    def process(tick_index, received, collected):
        position = jnp.clip(tick_index - section_index, 0, unit_count - 1)
        arriving = lax.dynamic_index_in_dim(
            units, jnp.minimum(tick_index, unit_count - 1), 0, keepdims=False
        )
        current = jnp.where(section_index == 0, arriving, received)
        ids_here = lax.dynamic_index_in_dim(unit_ids, position, 0, keepdims=False)
        live_here = lax.dynamic_index_in_dim(unit_live, position, 0, keepdims=False)
        produced = block_step(
            current,
            ids_here,
            live_here,
            gain_full,
            up_weight,
            down_weight,
            shrink_weight,
            expand_weight,
        )
        lag = tick_index - section_index
        in_window = jnp.logical_and(lag >= 0, lag < unit_count)
        placed = lax.dynamic_update_index_in_dim(collected, produced, position, 0)
        return (produced, jnp.where(in_window, placed, collected))

    def one_tick(tick_index, state):
        produced, collected = process(tick_index, state[0], state[1])
        return (shifted(produced, "pipe", 1), collected)

    start_state = (jnp.zeros_like(units[0]), jnp.zeros_like(units))
    received, collected = lax.fori_loop(0, tick_total - 1, one_tick, start_state)
    produced, collected = process(tick_total - 1, received, collected)
    return collected


def per_device(
    hidden_entering,
    segment_adapter,
    segment_requests,
    section_norm_gain,
    up_matrix,
    down_matrix,
    adapter_reduce,
    adapter_expand,
):
    batch_list = hidden_entering.shape[0]
    row_count = hidden_entering.shape[1]
    col_count = hidden_entering.shape[2]
    hidden = up_matrix.shape[1]
    fits = 2 * hidden * col_count * 2 * lax.axis_size("tp") < VMEM_BYTES - 7 * 2**20
    whole_pieces = col_count % PIECE == 0 and hidden % PIECE == 0 and hidden >= 4 * PIECE
    if batch_list == 1 and whole_pieces and fits and row_count <= 128:
        produced = fused_sections(
            hidden_entering[0],
            segment_adapter[0],
            segment_requests[0],
            section_norm_gain[0],
            up_matrix[0],
            down_matrix[0],
            adapter_reduce[0],
            adapter_expand[0],
        )
        return produced.reshape(1, batch_list, row_count, col_count)
    collected = run_window(
        hidden_entering,
        segment_adapter,
        segment_requests,
        section_norm_gain[0],
        up_matrix[0],
        down_matrix[0],
        adapter_reduce[0],
        adapter_expand[0],
    )
    return collected.reshape(1, batch_list, row_count, col_count)


def solution(mesh):
    return jax.shard_map(
        per_device,
        mesh=mesh,
        in_specs=(
            P("rep", None, "tp"),
            P("rep", None),
            P("rep", None),
            P("pipe", None),
            P("pipe", "tp", None),
            P("pipe", "tp", None),
            P("pipe", None, "tp"),
            P("pipe", None, "tp"),
        ),
        out_specs=P("pipe", "rep", None, "tp"),
        check_vma=False,
    )
```
